128 devices in a mesh: tm: 8 (over y, x_lo), space: 16 (over z, x_hi, core).
Axes of the slice: x: 4 (x_hi: 2, x_lo: 2; x = x_hi * 2 + x_lo), y: 4, z: 4, core: 2. Of those that a mesh axis runs over, the one named last changes fastest.
Arguments:
- queries: bfloat16 [16384, 4096], P(('tm', 'space')), may hold values from -20 to 20
- key_vectors: bfloat16 [16384, 4096], P(('tm', 'space')), may hold values from -20 to 20
- value_vectors: bfloat16 [16384, 4096], P(('tm', 'space')), may hold values from -6 to 6
- out_weight: bfloat16 [4096, 6144], P(None, 'space'), may hold values from -0.375 to 0.375
- frame_mask: int32 [8, 8], replicated, may hold values 0 or 1
Outputs:
- projected: bfloat16 [16384, 6144], P('tm', 'space')
The draws below stay inside these ranges and needn't reach their ends.
All inputs are finite; a program needn't handle non-finite values.
Results may differ from the reference program's by a relative error of at most 0.0075.
Values may be sent and summed in bfloat16 or wider, within the bound.
A program may use at most 128 MiB of HBM per device.

```python
import math
import jax
import jax.numpy as jnp
from jax import lax

D = 6144
HD = 128
HEADS = 32
TOK_DEV = 128
WIN = 1
BLOCKS = 8
TOKENS = 16384
N_TM = 8
N_SPACE = 16


def pair_draw(key):
    base = jax.random.fold_in(key, 7193)
    first_key, second_key = jax.random.split(base, 2)
    width = HEADS * HD
    query_draw = 2.0 * jax.random.truncated_normal(first_key, -4.0, 4.0, (TOKENS, width), jnp.float32)
    key_draw = jax.random.truncated_normal(second_key, -4.0, 4.0, (TOKENS, width), jnp.float32)
    return (query_draw, key_draw)


def draw_queries(key, part):
    return pair_draw(key)[0].astype(jnp.bfloat16)


def draw_key_vectors(key, part):
    return pair_draw(key)[1].astype(jnp.bfloat16)


def set_ends(drawn, own_key, least, top_value):
    extent = drawn.shape
    index_at = [jax.random.randint(jax.random.fold_in(own_key, axis), (), 0, extent[axis]) for axis in range(len(extent))]
    drawn = drawn.at[tuple(index_at)].set(least)
    longest = extent.index(max(extent))
    index_at[longest] = (index_at[longest] + 1) % extent[longest]
    return drawn.at[tuple(index_at)].set(top_value)


def block_scale(key, dims, cuts, least, largest):
    gain, own = 1.0, jax.random.fold_in(key, 6)
    for axis_at, blocks in cuts:
        draws = jnp.exp(jax.random.uniform(jax.random.fold_in(own, axis_at), (blocks,), jnp.float32, least / len(cuts), largest / len(cuts)))
        gain = gain * jnp.repeat(draws, dims[axis_at] // blocks).reshape([-1 if axis == axis_at else 1 for axis in range(len(dims))])
    return gain


def noise(key, shape, scale, limit, shards=(), kind=jnp.bfloat16):
    drawn = scale * jax.random.normal(key, shape, jnp.float32)
    if shards:
        drawn = drawn * block_scale(key, shape, shards, -0.22, 0.18)
    return jnp.clip(drawn, -limit, limit).astype(kind)


def setup_inputs(seed: int = 0) -> dict:
    keys = jax.random.split(jax.random.key(seed), 6)
    return {
        "queries": draw_queries(jax.random.fold_in(keys[5], 71), 0),
        "key_vectors": draw_key_vectors(jax.random.fold_in(keys[5], 71), 0),
        "value_vectors": noise(keys[2], (TOKENS, HEADS * HD), 1.0, 6.0, ((0, 128),)),
        "out_weight": noise(keys[3], (HEADS * HD, D), (HEADS * HD // 16) ** -0.5, 0.375, ((1, 16),)),
        "frame_mask": set_ends((jax.random.randint(keys[4], (BLOCKS, BLOCKS), 0, 5) < 4).astype(jnp.int32), jax.random.fold_in(keys[4], 1), 0, 1),
    }


def reference(queries, key_vectors, value_vectors, out_weight, frame_mask):
    block_tokens = TOK_DEV * N_SPACE
    scale_factor = 1.0 / math.sqrt(HD)
    pieces = []
    for frame_index in range(N_TM):
        block_list = [(frame_index + offset) % N_TM for offset in range(-WIN, WIN + 1)]
        query_rows = queries[frame_index * block_tokens:(frame_index + 1) * block_tokens]
        query_rows = query_rows.reshape(block_tokens, HEADS, HD).transpose(1, 0, 2)
        key_rows = jnp.concatenate([key_vectors[b * block_tokens:(b + 1) * block_tokens] for b in block_list], axis=0)
        key_rows = key_rows.reshape(-1, HEADS, HD).transpose(1, 0, 2)
        value_rows = jnp.concatenate([value_vectors[b * block_tokens:(b + 1) * block_tokens] for b in block_list], axis=0)
        value_rows = value_rows.reshape(-1, HEADS, HD).transpose(1, 0, 2)
        owners = jnp.concatenate([jnp.full((block_tokens,), b, jnp.int32) for b in block_list])
        mask_bits = frame_mask[frame_index][owners]
        allowed = (owners == frame_index) | (mask_bits == 1)

        def one_head(head_trio):
            query_head, key_head, value_head = head_trio
            scores = jnp.dot(query_head, key_head.T, preferred_element_type=jnp.float32) * scale_factor
            scores = jnp.where(allowed[None, :], scores, -jnp.inf)
            row_top = lax.optimization_barrier(jnp.max(scores, axis=1, keepdims=True))
            exp_terms = jnp.where(allowed[None, :], jnp.exp(scores - row_top), 0.0)
            totals = lax.optimization_barrier(jnp.sum(exp_terms, axis=1, keepdims=True))
            mixed = jnp.dot(exp_terms.astype(jnp.bfloat16), value_head, preferred_element_type=jnp.float32)
            return mixed / totals
        heads_out = lax.map(one_head, (query_rows, key_rows, value_rows))
        attended = heads_out.transpose(1, 0, 2).reshape(block_tokens, HEADS * HD).astype(jnp.bfloat16)
        pieces.append(jnp.dot(attended, out_weight, preferred_element_type=jnp.float32).astype(jnp.bfloat16))
    return jnp.concatenate(pieces, axis=0)
```

```python
import functools
import math

import jax
import jax.numpy as jnp
from jax import lax
from jax.experimental import pallas as pl
from jax.experimental.pallas import tpu as pltpu
from jax.sharding import PartitionSpec as P

MESH = pl.DeviceIdType.MESH
HD = 128
HEADS = 32
TOK = 128
BT = 2048
TQ = 256
KC = 512
SLOPE = math.log2(math.e) / math.sqrt(HD)
BIG = 1e30


def place():
    tm = lax.axis_index("tm")
    sp = lax.axis_index("space")
    return tm, sp, tm // 2, tm % 2


def taken(ref, sem):
    pltpu.make_async_copy(ref, ref, sem).wait()


def attend_tile(q, k_all, v_all, scores, base, bits):
    chunks = BT // KC
    top = None
    for j in range(3):
        part = None
        for c in range(chunks):
            off = j * BT + c * KC
            s = lax.dot_general(
                q, k_all[pl.ds(base + off, KC), :], (((1,), (1,)), ((), ())),
                preferred_element_type=jnp.float32,
            )
            scores[:, off:off + KC] = s
            for lane in range(0, KC, 128):
                piece = s[:, lane:lane + 128]
                part = piece if part is None else jnp.maximum(part, piece)
        if bits[j] is not None:
            part = jnp.where(bits[j], part, -jnp.inf)
        top = part if top is None else jnp.maximum(top, part)
    top = jnp.max(top, axis=1, keepdims=True)
    acc = None
    total = None
    for j in range(3):
        sub = top if bits[j] is None else jnp.where(bits[j], top, BIG)
        for c in range(chunks):
            off = j * BT + c * KC
            p = jnp.exp2((scores[:, off:off + KC] - sub) * SLOPE)
            for lane in range(0, KC, 128):
                piece = p[:, lane:lane + 128]
                total = piece if total is None else total + piece
            d = jnp.dot(
                p.astype(jnp.bfloat16), v_all[pl.ds(base + off, KC), :],
                preferred_element_type=jnp.float32,
            )
            acc = d if acc is None else acc + d
    return (acc / jnp.sum(total, axis=1, keepdims=True)).astype(jnp.bfloat16)


def exchange_kernel(
    q_src, k_src, v_src, q_hbm, k_hbm, v_hbm, mask_ref, att_ref,
    q_all, k_all, v_all, scores, sent, landed, passed_sem, came_sem,
):
    tm, sp, y, xl = place()
    me = xl * 16 + sp
    up = ((y + 1) % 4) * 2 + xl
    down = ((y + 3) % 4) * 2 + xl

    barrier = pltpu.get_barrier_semaphore()

    def greet(i, carry):
        p = (me + i) % 32
        pl.semaphore_signal(barrier, inc=1, device_id=(y * 2 + p // 16, p % 16), device_id_type=MESH)
        return carry

    lax.fori_loop(1, 32, greet, 0)
    pl.semaphore_signal(barrier, inc=1, device_id=(up, sp), device_id_type=MESH)
    pl.semaphore_signal(barrier, inc=1, device_id=(down, sp), device_id_type=MESH)
    pl.semaphore_wait(barrier, 33)

    mine = pl.ds(pl.multiple_of((sp * 2 + xl) * HD, HD), HD)
    plan = ((k_src, k_hbm, k_all, BT), (v_src, v_hbm, v_all, BT), (q_src, q_hbm, q_all, 0))
    for n, (src, hbm, dst, first) in enumerate(plan):
        rows = pl.ds(pl.multiple_of(first + me * TOK, TOK), TOK)
        pltpu.make_async_copy(hbm.at[:, mine], dst.at[rows, :], landed.at[n]).start()

        def send(i, carry, src=src, dst=dst, rows=rows, n=n):
            p = (me + i) % 32
            theirs = pl.ds(pl.multiple_of(((p % 16) * 2 + p // 16) * HD, HD), HD)
            pltpu.make_async_remote_copy(
                src_ref=src.at[:, theirs], dst_ref=dst.at[rows, :],
                send_sem=sent.at[n], recv_sem=landed.at[n],
                device_id=(y * 2 + p // 16, p % 16), device_id_type=MESH,
            ).start()
            return carry

        lax.fori_loop(1, 32, send, 0)

    hops = []
    for n, buf in enumerate((k_all, v_all)):
        taken(buf.at[BT:3 * BT, :], landed.at[n])
        for way, (there, src, dst) in enumerate(((up, 2 * BT, 0), (down, BT, 3 * BT))):
            hop = pltpu.make_async_remote_copy(
                src_ref=buf.at[src:src + BT, :], dst_ref=buf.at[dst:dst + BT, :],
                send_sem=passed_sem.at[2 * n + way], recv_sem=came_sem.at[2 * n + way],
                device_id=(there, sp), device_id_type=MESH,
            )
            hop.start()
            hops.append(hop)
    taken(q_all, landed.at[2])
    for hop in hops:
        hop.wait()
    for n in range(3):
        taken(q_all.at[0:31 * TOK, :], sent.at[n])

    per = BT // TQ

    def tile(t, carry):
        half = t // per
        block = y * 2 + half
        before = mask_ref[block, (block + 7) % 8] == 1
        after = mask_ref[block, (block + 1) % 8] == 1
        rows = pl.ds(pl.multiple_of(t * TQ, TQ), TQ)
        base = pl.multiple_of(half * BT, BT)
        att_ref[rows, :] = attend_tile(q_all[rows, :], k_all, v_all, scores, base, (before, None, after))
        return carry

    lax.fori_loop(0, 2 * per, tile, 0)


def exchange_and_attend(queries, key_vectors, value_vectors, frame_mask):
    vmem = pl.BlockSpec(memory_space=pltpu.VMEM)
    hbm = pl.BlockSpec(memory_space=pl.ANY)
    return pl.pallas_call(
        exchange_kernel,
        name="exchange_attend",
        out_shape=jax.ShapeDtypeStruct((2 * BT, HD), jnp.bfloat16),
        in_specs=[vmem] * 3 + [hbm] * 3 + [pl.BlockSpec(memory_space=pltpu.SMEM)],
        out_specs=vmem,
        scratch_shapes=[
            pltpu.VMEM((2 * BT, HD), jnp.bfloat16),
            pltpu.VMEM((4 * BT, HD), jnp.bfloat16),
            pltpu.VMEM((4 * BT, HD), jnp.bfloat16),
            pltpu.VMEM((TQ, 3 * BT), jnp.float32),
            pltpu.SemaphoreType.DMA((3,)),
            pltpu.SemaphoreType.DMA((3,)),
            pltpu.SemaphoreType.DMA((4,)),
            pltpu.SemaphoreType.DMA((4,)),
        ],
        compiler_params=pltpu.CompilerParams(
            collective_id=0, has_side_effects=True, vmem_limit_bytes=48 * 2**20
        ),
        cost_estimate=pl.CostEstimate(flops=13 * 10**9, bytes_accessed=8 * 2**20, transcendentals=25 * 10**6),
    )(queries, key_vectors, value_vectors, queries, key_vectors, value_vectors, frame_mask)


ROWS = BT // 2
COLS = 384
PART = 256


def project_kernel(
    att_hbm, w_hbm, out_ref, got, w_all, acc, theirs,
    near_send, near_recv, far_send, far_recv, relay_send, relay_recv, w_mine, w_send, w_recv, o_send, o_recv,
):
    tm, sp, y, xl = place()
    z = sp // 4
    xh = (sp // 2) % 2
    core = sp % 2
    head = sp * 2 + xl
    above = ((z + 1) % 4) * 4 + xh * 2 + core
    below = ((z + 3) % 4) * 4 + xh * 2 + core
    partner = sp + 1 - 2 * core

    barrier = pltpu.get_barrier_semaphore()
    near = xh * 4 + core * 2 + xl

    def row_device(p):
        return (y * 2 + p % 2, z * 4 + (p // 4) * 2 + (p // 2) % 2)

    def greet(i, carry):
        pl.semaphore_signal(barrier, inc=1, device_id=row_device((near + i) % 8), device_id_type=MESH)
        return carry

    lax.fori_loop(1, 8, greet, 0)
    pl.semaphore_signal(barrier, inc=1, device_id=(tm, above), device_id_type=MESH)
    pl.semaphore_signal(barrier, inc=1, device_id=(tm, below), device_id_type=MESH)
    pl.semaphore_wait(barrier, 9)

    def rows_of(p):
        quarter = (p % 2) * 2 + (p // 2) % 2
        return pl.ds(pl.multiple_of(quarter * ROWS, ROWS), ROWS)

    own = pltpu.make_async_copy(att_hbm.at[rows_of(near), :], got.at[head], near_recv.at[near])
    own.start()

    def send(i, carry):
        p = (near + i) % 8
        pltpu.make_async_remote_copy(
            src_ref=att_hbm.at[rows_of(p), :], dst_ref=got.at[head],
            send_sem=near_send, recv_sem=near_recv.at[near],
            device_id=row_device(p), device_id_type=MESH,
        ).start()
        return carry

    lax.fori_loop(1, 8, send, 0)

    mine = pl.ds(pl.multiple_of(core * COLS, COLS), COLS)
    w_own = pltpu.make_async_copy(w_hbm, w_all.at[:, mine], w_mine)
    w_own.start()
    w_copy = pltpu.make_async_remote_copy(
        src_ref=w_hbm, dst_ref=w_all.at[:, mine], send_sem=w_send, recv_sem=w_recv,
        device_id=(tm, partner), device_id_type=MESH,
    )
    w_copy.start()

    def onward(i, carry):
        p = (near + i) % 8
        slot = z * 8 + p
        taken(got.at[slot], near_recv.at[p])
        for way, there in enumerate((above, below)):
            pltpu.make_async_remote_copy(
                src_ref=got.at[slot], dst_ref=got.at[slot],
                send_sem=far_send, recv_sem=far_recv.at[way, p],
                device_id=(tm, there), device_id_type=MESH,
            ).start()
        return carry

    lax.fori_loop(0, 8, onward, 0)

    z_from_below = (z + 3) % 4
    z_from_above = (z + 1) % 4
    z_far = (z + 2) % 4

    w_own.wait()
    w_copy.wait()
    half = pl.multiple_of(core * ROWS, ROWS)
    cut = [pl.ds(pl.multiple_of(c * COLS, COLS), COLS) for c in (core, 1 - core)]

    def product(zz, first=False, last=False):
        def rows(r, carry):
            part = pl.ds(pl.multiple_of(r * PART, PART), PART)
            lhs = jnp.concatenate([got[zz * 8 + i, part, :] for i in range(8)], axis=1)
            k_rows = pl.ds(pl.multiple_of(zz * 1024, 1024), 1024)
            d = jnp.dot(lhs, w_all[k_rows, :], preferred_element_type=jnp.float32)
            acc[part, :] = d if first else acc[part, :] + d
            if last:
                theirs[part, :] = acc[part, cut[1]].astype(jnp.bfloat16)
                out_ref[pl.ds(pl.multiple_of(half + r * PART, PART), PART), :] = acc[part, cut[0]].astype(jnp.bfloat16)
            return carry

        lax.fori_loop(0, ROWS // PART, rows, 0)

    product(z, first=True)

    def pass_on(i, carry):
        for way, (zz, there) in enumerate(((z_from_below, above), (z_from_above, below))):
            p = i + 4 * way
            slot = zz * 8 + p
            taken(got.at[slot], far_recv.at[way, p])
            pltpu.make_async_remote_copy(
                src_ref=got.at[slot], dst_ref=got.at[slot],
                send_sem=relay_send, recv_sem=relay_recv,
                device_id=(tm, there), device_id_type=MESH,
            ).start()
        return carry

    lax.fori_loop(0, 4, pass_on, 0)

    def rest(i, carry):
        for way, zz in enumerate((z_from_below, z_from_above)):
            p = i + 4 * (1 - way)
            taken(got.at[zz * 8 + p], far_recv.at[way, p])
        return carry

    lax.fori_loop(0, 4, rest, 0)
    product(z_from_below)
    product(z_from_above)
    taken(got.at[pl.ds(z_far * 8, 8)], relay_recv)
    product(z_far, last=True)
    o_copy = pltpu.make_async_remote_copy(
        src_ref=theirs, dst_ref=out_ref.at[pl.ds(half, ROWS), :], send_sem=o_send, recv_sem=o_recv,
        device_id=(tm, partner), device_id_type=MESH,
    )
    o_copy.start()
    o_copy.wait()
    taken(got.at[0:7], near_send)
    taken(got.at[0:16], far_send)
    taken(got.at[0:8], relay_send)


def gather_and_project(att, out_weight):
    vmem = pl.BlockSpec(memory_space=pltpu.VMEM)
    hbm = pl.BlockSpec(memory_space=pl.ANY)
    dma = pltpu.SemaphoreType.DMA
    return pl.pallas_call(
        project_kernel,
        name="gather_project",
        out_shape=jax.ShapeDtypeStruct((BT, COLS), jnp.bfloat16),
        in_specs=[hbm, hbm],
        out_specs=vmem,
        scratch_shapes=[
            pltpu.VMEM((HEADS, ROWS, HD), jnp.bfloat16),
            pltpu.VMEM((HEADS * HD, 2 * COLS), jnp.bfloat16),
            pltpu.VMEM((ROWS, 2 * COLS), jnp.float32),
            pltpu.VMEM((ROWS, COLS), jnp.bfloat16),
            dma, dma((8,)), dma, dma((2, 8)), dma, dma, dma, dma, dma, dma, dma,
        ],
        compiler_params=pltpu.CompilerParams(
            collective_id=1, has_side_effects=True, vmem_limit_bytes=48 * 2**20
        ),
        cost_estimate=pl.CostEstimate(flops=64 * 10**8, bytes_accessed=8 * 2**20, transcendentals=0),
    )(att, out_weight)


def body(queries, key_vectors, value_vectors, out_weight, frame_mask):
    att = exchange_and_attend(queries, key_vectors, value_vectors, frame_mask)
    return gather_and_project(att, out_weight)


def solution(mesh):
    in_specs = (
        P(("tm", "space"), None),
        P(("tm", "space"), None),
        P(("tm", "space"), None),
        P(None, "space"),
        P(),
    )
    return jax.shard_map(body, mesh=mesh, in_specs=in_specs, out_specs=P("tm", "space"), check_vma=False)
```

```python
import functools
import math

import jax
import jax.numpy as jnp
from jax import lax
from jax.experimental import pallas as pl
from jax.experimental.pallas import tpu as pltpu
from jax.sharding import PartitionSpec as P

MESH = pl.DeviceIdType.MESH
HD = 128
HEADS = 32
TOK = 128
BT = 2048
TQ = 256
KC = 512
COLS = 384
ROWS = 512
STEPS = 16
SLOPE = math.log2(math.e) / math.sqrt(HD)
BIG = 1e30


def place():
    tm = lax.axis_index("tm")
    sp = lax.axis_index("space")
    return tm, sp, tm // 2, tm % 2


def taken(ref, sem):
    pltpu.make_async_copy(ref, ref, sem).wait()


def attend_tile(q, k_all, v_all, scores, base, bits):
    chunks = BT // KC
    top = None
    for j in range(3):
        part = None
        for c in range(chunks):
            off = j * BT + c * KC
            s = lax.dot_general(
                q, k_all[pl.ds(base + off, KC), :], (((1,), (1,)), ((), ())),
                preferred_element_type=jnp.float32,
            )
            scores[:, off:off + KC] = s
            for lane in range(0, KC, 128):
                piece = s[:, lane:lane + 128]
                part = piece if part is None else jnp.maximum(part, piece)
        if bits[j] is not None:
            part = jnp.where(bits[j], part, -jnp.inf)
        top = part if top is None else jnp.maximum(top, part)
    top = jnp.max(top, axis=1, keepdims=True)
    acc = None
    total = None
    for j in range(3):
        sub = top if bits[j] is None else jnp.where(bits[j], top, BIG)
        for c in range(chunks):
            off = j * BT + c * KC
            p = jnp.exp2((scores[:, off:off + KC] - sub) * SLOPE)
            for lane in range(0, KC, 128):
                piece = p[:, lane:lane + 128]
                total = piece if total is None else total + piece
            d = jnp.dot(
                p.astype(jnp.bfloat16), v_all[pl.ds(base + off, KC), :],
                preferred_element_type=jnp.float32,
            )
            acc = d if acc is None else acc + d
    return (acc / jnp.sum(total, axis=1, keepdims=True)).astype(jnp.bfloat16)


def kernel(
    q_src, k_src, v_src, q_hbm, k_hbm, v_hbm, w_hbm, mask_ref, out_ref,
    q_all, k_all, v_all, scores, att, got, w_all, done,
    sent, landed, passed_sem, came_sem, near_send, near_recv, far_send, far_recv,
    w_mine, w_send, w_recv, o_send, o_recv,
):
    tm, sp, y, xl = place()
    z = sp // 4
    xh = (sp // 2) % 2
    core = sp % 2
    me = xl * 16 + sp

    def at_y(step):
        return (((y + step) % 4) * 2 + xl, sp)

    def at_z(step):
        return (tm, ((z + step) % 4) * 4 + sp % 4)

    barrier = pltpu.get_barrier_semaphore()

    def greet(i, carry):
        p = (me + i) % 32
        pl.semaphore_signal(barrier, inc=1, device_id=(y * 2 + p // 16, p % 16), device_id_type=MESH)
        return carry

    lax.fori_loop(1, 32, greet, 0)
    for step in (1, 2, 3):
        pl.semaphore_signal(barrier, inc=1, device_id=at_y(step), device_id_type=MESH)
    pl.semaphore_wait(barrier, 34)

    mine = pl.ds(pl.multiple_of((sp * 2 + xl) * HD, HD), HD)
    plan = ((k_src, k_hbm, k_all, BT), (v_src, v_hbm, v_all, BT), (q_src, q_hbm, q_all, 0))
    for n, (src, hbm, dst, first) in enumerate(plan):
        rows = pl.ds(pl.multiple_of(first + me * TOK, TOK), TOK)
        pltpu.make_async_copy(hbm.at[:, mine], dst.at[rows, :], landed.at[n]).start()

        def send(i, carry, src=src, dst=dst, rows=rows, n=n):
            p = (me + i) % 32
            theirs = pl.ds(pl.multiple_of(((p % 16) * 2 + p // 16) * HD, HD), HD)
            pltpu.make_async_remote_copy(
                src_ref=src.at[:, theirs], dst_ref=dst.at[rows, :],
                send_sem=sent.at[n], recv_sem=landed.at[n],
                device_id=(y * 2 + p // 16, p % 16), device_id_type=MESH,
            ).start()
            return carry

        lax.fori_loop(1, 32, send, 0)

    def columns(g):
        return pl.ds(pl.multiple_of(g * COLS, COLS), COLS)

    g_me = xh * 2 + core
    g_far = (1 - xh) * 2 + core
    quarter = pl.ds(pl.multiple_of(y * 1024, 1024), 1024)
    partner = (tm, sp + 1 - 2 * core)
    across = (y * 2 + 1 - xl, z * 4 + g_far)
    w_own = pltpu.make_async_copy(w_hbm, w_all.at[:, columns(g_me)], w_mine)
    w_own.start()
    w_near = pltpu.make_async_remote_copy(
        src_ref=w_hbm, dst_ref=w_all.at[:, columns(g_me)], send_sem=w_send.at[0], recv_sem=w_recv.at[0],
        device_id=partner, device_id_type=MESH,
    )
    w_near.start()
    w_first = pltpu.make_async_remote_copy(
        src_ref=w_hbm.at[quarter, :], dst_ref=w_all.at[quarter, columns(g_me)],
        send_sem=w_send.at[1], recv_sem=w_recv.at[1], device_id=across, device_id_type=MESH,
    )
    w_first.start()

    hops = []
    for n, buf in enumerate((k_all, v_all)):
        taken(buf.at[BT:3 * BT, :], landed.at[n])
        for way, (step, src, dst) in enumerate(((1, 2 * BT, 0), (3, BT, 3 * BT))):
            hop = pltpu.make_async_remote_copy(
                src_ref=buf.at[src:src + BT, :], dst_ref=buf.at[dst:dst + BT, :],
                send_sem=passed_sem.at[2 * n + way], recv_sem=came_sem.at[2 * n + way],
                device_id=at_y(step), device_id_type=MESH,
            )
            hop.start()
            hops.append(hop)
    taken(q_all, landed.at[2])
    for hop in hops:
        hop.wait()
    for n in range(3):
        taken(q_all.at[0:31 * TOK, :], sent.at[n])

    turn = core * 4 + xh * 2 + xl
    slot = xh * 4 + core * 2 + xl

    def along_z(chunk):
        rows = pl.ds(chunk * TQ, TQ)
        taken(got.at[0, 0:7, 0:TQ, :], near_recv.at[chunk])
        for step in (1, 3, 2):
            pltpu.make_async_remote_copy(
                src_ref=got.at[z, :, rows, :], dst_ref=got.at[z, :, rows, :],
                send_sem=far_send, recv_sem=far_recv.at[chunk],
                device_id=at_z(step), device_id_type=MESH,
            ).start()

    def tile(s, carry):
        chunk = s // 8
        to_core = (s % 8) // 4
        half = s % 2
        to_xh = (s % 4) // 2
        block = y * 2 + half
        before = mask_ref[block, (block + 7) % 8] == 1
        after = mask_ref[block, (block + 1) % 8] == 1
        rows = pl.ds(pl.multiple_of(half * BT + (to_xh * 2 + to_core) * ROWS + chunk * TQ, TQ), TQ)
        base = pl.multiple_of(half * BT, BT)
        there = pl.ds(pl.multiple_of(chunk * TQ, TQ), TQ)
        result = attend_tile(q_all[rows, :], k_all, v_all, scores, base, (before, None, after))

        @pl.when(s % 8 == turn)
        def _():
            got[z, slot, there, :] = result

        @pl.when(s % 8 != turn)
        def _():
            att[rows, :] = result
            pltpu.make_async_remote_copy(
                src_ref=att.at[rows, :], dst_ref=got.at[z, slot, there, :],
                send_sem=near_send, recv_sem=near_recv.at[chunk],
                device_id=(y * 2 + half, z * 4 + to_xh * 2 + to_core), device_id_type=MESH,
            ).start()

        for c in (0, 1):
            @pl.when(s == c * 8 + turn + 2)
            def _(c=c):
                along_z(c)

        @pl.when(s == 4)
        def _():
            w_first.wait()
            for n, step in enumerate((1, 3, 2)):
                pltpu.make_async_remote_copy(
                    src_ref=w_all.at[quarter, columns(g_far)], dst_ref=w_all.at[quarter, columns(g_far)],
                    send_sem=w_send.at[2], recv_sem=w_recv.at[2], device_id=at_y(step), device_id_type=MESH,
                ).start()

        return carry

    lax.fori_loop(0, STEPS, tile, 0)

    @pl.when(turn >= 6)
    def _():
        along_z(1)

    w_own.wait()
    w_near.wait()
    taken(w_all.at[0:3072, 0:COLS], w_recv.at[2])
    w_last = pltpu.make_async_remote_copy(
        src_ref=w_all.at[:, columns(g_far)], dst_ref=w_all.at[:, columns(g_far)],
        send_sem=w_send.at[3], recv_sem=w_recv.at[3], device_id=partner, device_id_type=MESH,
    )
    w_last.start()
    w_last.wait()

    for chunk in (0, 1):
        rows = pl.ds(chunk * TQ, TQ)
        out_rows = pl.ds(pl.multiple_of(g_me * ROWS + chunk * TQ, TQ), TQ)
        taken(got.at[0:3, :, 0:TQ, :], far_recv.at[chunk])
        lhs = jnp.concatenate([got[i // 8, i % 8, rows, :] for i in range(HEADS)], axis=1)
        for pair in (1, 0):
            side = (xh + pair) % 2
            wide = pl.ds(pl.multiple_of(side * 2 * COLS, 2 * COLS), 2 * COLS)
            d = jnp.dot(lhs, w_all[:, wide], preferred_element_type=jnp.float32).astype(jnp.bfloat16)
            for c in (0, 1):
                g = side * 2 + c
                block = d[:, c * COLS:(c + 1) * COLS]

                @pl.when(g == g_me)
                def _(block=block):
                    out_ref[out_rows, :] = block

                @pl.when(g != g_me)
                def _(block=block, g=g, n=chunk * 4 + pair * 2 + c, c=c, side=side):
                    done[n] = block
                    pltpu.make_async_remote_copy(
                        src_ref=done.at[n], dst_ref=out_ref.at[out_rows, :],
                        send_sem=o_send, recv_sem=o_recv,
                        device_id=(tm, z * 4 + g), device_id_type=MESH,
                    ).start()

    taken(out_ref.at[0:6 * TQ, :], o_recv)
    taken(out_ref.at[0:6 * TQ, :], o_send)
    taken(q_all.at[0:14 * TQ, :], near_send)
    taken(got.at[0:3], far_send)
    taken(w_all.at[0:3072, 0:COLS], w_send.at[2])


def body(queries, key_vectors, value_vectors, out_weight, frame_mask):
    vmem = pl.BlockSpec(memory_space=pltpu.VMEM)
    hbm = pl.BlockSpec(memory_space=pl.ANY)
    dma = pltpu.SemaphoreType.DMA
    bf16 = jnp.bfloat16
    return pl.pallas_call(
        kernel,
        name="layer",
        out_shape=jax.ShapeDtypeStruct((BT, COLS), bf16),
        in_specs=[vmem] * 3 + [hbm] * 4 + [pl.BlockSpec(memory_space=pltpu.SMEM)],
        out_specs=vmem,
        scratch_shapes=[
            pltpu.VMEM((2 * BT, HD), bf16),
            pltpu.VMEM((4 * BT, HD), bf16),
            pltpu.VMEM((4 * BT, HD), bf16),
            pltpu.VMEM((TQ, 3 * BT), jnp.float32),
            pltpu.VMEM((2 * BT, HD), bf16),
            pltpu.VMEM((4, 8, ROWS, HD), bf16),
            pltpu.VMEM((HEADS * HD, 4 * COLS), bf16),
            pltpu.VMEM((8, TQ, COLS), bf16),
            dma((3,)), dma((3,)), dma((4,)), dma((4,)), dma, dma((2,)), dma, dma((2,)),
            dma, dma((4,)), dma((4,)), dma, dma,
        ],
        compiler_params=pltpu.CompilerParams(
            collective_id=0, has_side_effects=True, vmem_limit_bytes=60 * 2**20
        ),
        cost_estimate=pl.CostEstimate(flops=19 * 10**9, bytes_accessed=8 * 2**20, transcendentals=25 * 10**6),
    )(queries, key_vectors, value_vectors, queries, key_vectors, value_vectors, out_weight, frame_mask)


def solution(mesh):
    in_specs = (
        P(("tm", "space"), None),
        P(("tm", "space"), None),
        P(("tm", "space"), None),
        P(None, "space"),
        P(),
    )
    return jax.shard_map(body, mesh=mesh, in_specs=in_specs, out_specs=P("tm", "space"), check_vma=False)
```

```python
import functools
import math

import jax
import jax.numpy as jnp
from jax import lax
from jax.experimental import pallas as pl
from jax.experimental.pallas import tpu as pltpu
from jax.sharding import PartitionSpec as P

MESH = pl.DeviceIdType.MESH
HD = 128
HEADS = 32
TOK = 128
BT = 2048
TQ = 256
KC = 512
COLS = 384
ROWS = 512
STEPS = 16
EARLY = 6
RELAY = 4
SLOPE = math.log2(math.e) / math.sqrt(HD)
BIG = 1e30


def place():
    tm = lax.axis_index("tm")
    sp = lax.axis_index("space")
    return tm, sp, tm // 2, tm % 2


def taken(ref, sem):
    pltpu.make_async_copy(ref, ref, sem).wait()


def attend(q, k_all, v_all, scores, blocks, known=None):
    chunks = BT // KC
    top = None
    for j, (base, bit) in enumerate(blocks):
        part = None
        for c in range(chunks):
            off = j * BT + c * KC
            s = lax.dot_general(
                q, k_all[pl.ds(base + c * KC, KC), :], (((1,), (1,)), ((), ())),
                preferred_element_type=jnp.float32,
            )
            scores[:, off:off + KC] = s
            for lane in range(0, KC, 128):
                piece = s[:, lane:lane + 128]
                part = piece if part is None else jnp.maximum(part, piece)
        if bit is not None:
            part = jnp.where(bit, part, -jnp.inf)
        top = part if top is None else jnp.maximum(top, part)
    top = jnp.max(top, axis=1, keepdims=True)
    acc = None
    total = None
    if known is not None:
        old_top, total, acc = known
        top = jnp.maximum(top, old_top[:, 0:1])
        shrink = jnp.exp2((old_top - top) * SLOPE)
        total = total * shrink
        acc = acc * shrink
    for j, (base, bit) in enumerate(blocks):
        sub = top if bit is None else jnp.where(bit, top, BIG)
        for c in range(chunks):
            off = j * BT + c * KC
            p = jnp.exp2((scores[:, off:off + KC] - sub) * SLOPE)
            for lane in range(0, KC, 128):
                piece = p[:, lane:lane + 128]
                total = piece if total is None else total + piece
            d = jnp.dot(
                p.astype(jnp.bfloat16), v_all[pl.ds(base + c * KC, KC), :],
                preferred_element_type=jnp.float32,
            )
            acc = d if acc is None else acc + d
    return top, total, acc


def finish(total, acc):
    return (acc / jnp.sum(total, axis=1, keepdims=True)).astype(jnp.bfloat16)


def kernel(
    q_hbm, k_hbm, v_hbm, w_hbm, mask_ref, out_ref,
    q_all, k_all, v_all, scores, att, got, w_all, done, tile_out, early_top, early_total, early_acc,
    sent, landed, passed_sem, came_sem, near_send, near_recv, far_send, far_recv, relay_recv,
    w_mine, w_send, w_recv, o_send, o_recv, o_own,
):
    tm, sp, y, xl = place()
    z = sp // 4
    xh = (sp // 2) % 2
    core = sp % 2
    me = xl * 16 + sp

    def at_y(step):
        return (((y + step) % 4) * 2 + xl, sp)

    def at_z(step):
        return (tm, ((z + step) % 4) * 4 + sp % 4)

    barrier = pltpu.get_barrier_semaphore()

    def greet(i, carry):
        p = (me + i) % 32
        pl.semaphore_signal(barrier, inc=1, device_id=(y * 2 + p // 16, p % 16), device_id_type=MESH)
        return carry

    lax.fori_loop(1, 32, greet, 0)
    for step in (1, 2, 3):
        pl.semaphore_signal(barrier, inc=1, device_id=at_y(step), device_id_type=MESH)
    pl.semaphore_wait(barrier, 34)

    mine = pl.ds(pl.multiple_of((sp * 2 + xl) * HD, HD), HD)
    plan = ((k_hbm, k_all, BT), (v_hbm, v_all, BT), (q_hbm, q_all, 0))
    cuts = (1, 16, 32)

    def rows_at(n):
        return pl.ds(pl.multiple_of(plan[n][2] + me * TOK, TOK), TOK)

    def send_part(n, part):
        hbm, dst, first = plan[n]

        def send(i, carry):
            p = (me + i) % 32
            theirs = pl.ds(pl.multiple_of(((p % 16) * 2 + p // 16) * HD, HD), HD)
            pltpu.make_async_remote_copy(
                src_ref=hbm.at[:, theirs], dst_ref=dst.at[rows_at(n), :],
                send_sem=sent.at[n, part], recv_sem=landed.at[n],
                device_id=(y * 2 + p // 16, p % 16), device_id_type=MESH,
            ).start()
            return carry

        lax.fori_loop(cuts[part], cuts[part + 1], send, 0)

    def sent_part(n, part):
        taken(q_all.at[0:(cuts[part + 1] - cuts[part]) * TOK, :], sent.at[n, part])

    hops = []

    def hop_on(n):
        buf = plan[n][1]
        taken(buf.at[BT:3 * BT, :], landed.at[n])
        for way, (step, src, dst) in enumerate(((1, 2 * BT, 0), (3, BT, 3 * BT))):
            hop = pltpu.make_async_remote_copy(
                src_ref=buf.at[src:src + BT, :], dst_ref=buf.at[dst:dst + BT, :],
                send_sem=passed_sem.at[2 * n + way], recv_sem=came_sem.at[2 * n + way],
                device_id=at_y(step), device_id_type=MESH,
            )
            hop.start()
            hops.append(hop)

    for n in range(3):
        pltpu.make_async_copy(plan[n][0].at[:, mine], plan[n][1].at[rows_at(n), :], landed.at[n]).start()
    send_part(0, 0)
    send_part(0, 1)
    for n in (0, 1):
        sent_part(n, 0)
        send_part(n + 1, 0)
        sent_part(n, 1)
        send_part(n + 1, 1)
        hop_on(n)

    def columns(n):
        return pl.ds(pl.multiple_of(n * COLS, COLS), COLS)

    near_cols = columns(2 + core)
    far_cols = columns(core)
    quarter = pl.ds(pl.multiple_of(y * 1024, 1024), 1024)
    g_me = xh * 2 + core
    partner = (tm, sp + 1 - 2 * core)
    across = (y * 2 + 1 - xl, z * 4 + (1 - xh) * 2 + core)
    w_first = pltpu.make_async_remote_copy(
        src_ref=w_hbm.at[quarter, :], dst_ref=w_all.at[quarter, far_cols],
        send_sem=w_send.at[1], recv_sem=w_recv.at[1], device_id=across, device_id_type=MESH,
    )
    w_first.start()
    w_own = pltpu.make_async_copy(w_hbm, w_all.at[:, near_cols], w_mine)
    w_own.start()
    w_near = pltpu.make_async_remote_copy(
        src_ref=w_hbm, dst_ref=w_all.at[:, near_cols], send_sem=w_send.at[0], recv_sem=w_recv.at[0],
        device_id=partner, device_id_type=MESH,
    )
    w_near.start()
    w_last = pltpu.make_async_remote_copy(
        src_ref=w_all.at[:, far_cols], dst_ref=w_all.at[:, far_cols],
        send_sem=w_send.at[3], recv_sem=w_recv.at[3], device_id=partner, device_id_type=MESH,
    )

    def spot(s):
        half = s % 2
        row = half * BT + ((s % 4) // 2 * 2 + (s % 8) // 4) * ROWS + s // 8 * TQ
        block = y * 2 + half
        before = mask_ref[block, (block + 7) % 8] == 1
        after = mask_ref[block, (block + 1) % 8] == 1
        return half, pl.ds(pl.multiple_of(row, TQ), TQ), before, after

    def early(s, carry):
        half, rows, before, after = spot(s)
        blocks = ((BT, (half == 0) | before), (2 * BT, (half == 1) | after))
        top, total, acc = attend(q_all[rows, :], k_all, v_all, scores, blocks)
        early_top[s] = jnp.broadcast_to(top, (TQ, HD))
        early_total[s] = total
        early_acc[s] = acc
        return carry

    taken(q_all, landed.at[2])
    lax.fori_loop(0, EARLY, early, 0)
    for hop in hops:
        hop.wait()
    sent_part(2, 0)
    sent_part(2, 1)

    turn = core * 4 + xh * 2 + xl
    slot = xh * 4 + core * 2 + xl

    def along_z(chunk):
        rows = pl.ds(chunk * TQ, TQ)
        taken(got.at[0, 0:7, 0:TQ, :], near_recv.at[chunk])
        for way, step in enumerate((1, 3)):
            pltpu.make_async_remote_copy(
                src_ref=got.at[z, :, rows, :], dst_ref=got.at[z, :, rows, :],
                send_sem=far_send, recv_sem=far_recv.at[2 * chunk + way],
                device_id=at_z(step), device_id_type=MESH,
            ).start()

    def relay_z(chunk):
        rows = pl.ds(chunk * TQ, TQ)
        for way, (come, step) in enumerate(((3, 1), (1, 3))):
            taken(got.at[0, :, 0:TQ, :], far_recv.at[2 * chunk + way])
            part = got.at[(z + come) % 4, 4 * way:4 * way + 4, rows, :]
            pltpu.make_async_remote_copy(
                src_ref=part, dst_ref=part, send_sem=far_send, recv_sem=relay_recv.at[chunk],
                device_id=at_z(step), device_id_type=MESH,
            ).start()

    def tile(s, carry):
        chunk = s // 8
        to_core = (s % 8) // 4
        half = s % 2
        to_xh = (s % 4) // 2
        _, rows, before, after = spot(s)
        base = pl.multiple_of(half * BT, BT)
        there = pl.ds(pl.multiple_of(chunk * TQ, TQ), TQ)

        @pl.when(s < EARLY)
        def _():
            n = jnp.minimum(s, EARLY - 1)
            last = pl.multiple_of(half * 3 * BT, BT)
            bit = ((half == 0) & before) | ((half == 1) & after)
            known = (early_top[n], early_total[n], early_acc[n])
            _, total, acc = attend(q_all[rows, :], k_all, v_all, scores, ((last, bit),), known)
            tile_out[...] = finish(total, acc)

        @pl.when(s >= EARLY)
        def _():
            blocks = ((base, before), (base + BT, None), (base + 2 * BT, after))
            _, total, acc = attend(q_all[rows, :], k_all, v_all, scores, blocks)
            tile_out[...] = finish(total, acc)

        result = tile_out[...]

        @pl.when(s % 8 == turn)
        def _():
            got[z, slot, there, :] = result

        @pl.when(s % 8 != turn)
        def _():
            att[rows, :] = result
            pltpu.make_async_remote_copy(
                src_ref=att.at[rows, :], dst_ref=got.at[z, slot, there, :],
                send_sem=near_send, recv_sem=near_recv.at[chunk],
                device_id=(y * 2 + half, z * 4 + to_xh * 2 + to_core), device_id_type=MESH,
            ).start()

        for c in (0, 1):
            @pl.when(s == c * 8 + turn + 1)
            def _(c=c):
                along_z(c)

            @pl.when(s == c * 8 + turn + RELAY)
            def _(c=c):
                relay_z(c)

        @pl.when(s == 2)
        def _():
            w_first.wait()
            for n, step in enumerate((1, 3, 2)):
                pltpu.make_async_remote_copy(
                    src_ref=w_all.at[quarter, far_cols], dst_ref=w_all.at[quarter, far_cols],
                    send_sem=w_send.at[2], recv_sem=w_recv.at[2], device_id=at_y(step), device_id_type=MESH,
                ).start()

        @pl.when(s == STEPS - 2)
        def _():
            taken(w_all.at[0:3072, 0:COLS], w_recv.at[2])
            w_last.start()

        return carry

    lax.fori_loop(0, STEPS, tile, 0)

    @pl.when(turn == 7)
    def _():
        along_z(1)

    w_own.wait()
    w_near.wait()
    w_last.wait()

    own_copies = []
    for chunk in (0, 1):
        rows = pl.ds(chunk * TQ, TQ)
        out_rows = pl.ds(pl.multiple_of(g_me * ROWS + chunk * TQ, TQ), TQ)

        def give(there, cols, chunk=chunk, out_rows=out_rows):
            pltpu.make_async_remote_copy(
                src_ref=done.at[chunk, :, cols], dst_ref=out_ref.at[out_rows, :],
                send_sem=o_send, recv_sem=o_recv,
                device_id=(tm, there), device_id_type=MESH,
            ).start()

        if chunk == 1:
            @pl.when(turn + 8 + RELAY > STEPS - 1)
            def _():
                relay_z(1)

        taken(got.at[0, :, 0:TQ, :], relay_recv.at[chunk])
        lhs = jnp.concatenate([got[i // 8, i % 8, rows, :] for i in range(HEADS)], axis=1)
        for n in range(3):
            wide = slice(n * 512, (n + 1) * 512)
            done[chunk, :, wide] = jnp.dot(lhs, w_all[:, wide], preferred_element_type=jnp.float32).astype(jnp.bfloat16)
            if n == 1:
                for c in (0, 1):
                    give(z * 4 + (1 - xh) * 2 + c, slice(c * COLS, (c + 1) * COLS))
        give(sp + 1 - 2 * core, columns(3 - core))
        own = pltpu.make_async_copy(done.at[chunk, :, near_cols], out_ref.at[out_rows, :], o_own.at[chunk])
        own.start()
        own_copies.append(own)

    for own in own_copies:
        own.wait()
    taken(done.at[:, :, 0:3 * COLS], o_recv)
    taken(done.at[:, :, 0:3 * COLS], o_send)
    taken(q_all.at[0:14 * TQ, :], near_send)
    taken(got.at[0:3], far_send)
    taken(w_all.at[0:3072, 0:COLS], w_send.at[2])


def body(queries, key_vectors, value_vectors, out_weight, frame_mask):
    hbm = pl.BlockSpec(memory_space=pl.ANY)
    dma = pltpu.SemaphoreType.DMA
    bf16 = jnp.bfloat16
    return pl.pallas_call(
        kernel,
        name="layer",
        out_shape=jax.ShapeDtypeStruct((BT, COLS), bf16),
        in_specs=[hbm] * 4 + [pl.BlockSpec(memory_space=pltpu.SMEM)],
        out_specs=hbm,
        scratch_shapes=[
            pltpu.VMEM((2 * BT, HD), bf16),
            pltpu.VMEM((4 * BT, HD), bf16),
            pltpu.VMEM((4 * BT, HD), bf16),
            pltpu.VMEM((TQ, 3 * BT), jnp.float32),
            pltpu.VMEM((2 * BT, HD), bf16),
            pltpu.VMEM((4, 8, ROWS, HD), bf16),
            pltpu.VMEM((HEADS * HD, 4 * COLS), bf16),
            pltpu.VMEM((2, TQ, 4 * COLS), bf16),
            pltpu.VMEM((TQ, HD), bf16),
            pltpu.VMEM((EARLY, TQ, HD), jnp.float32),
            pltpu.VMEM((EARLY, TQ, HD), jnp.float32),
            pltpu.VMEM((EARLY, TQ, HD), jnp.float32),
            dma((3, 2)), dma((3,)), dma((4,)), dma((4,)), dma, dma((2,)), dma, dma((4,)), dma((2,)),
            dma, dma((4,)), dma((4,)), dma, dma, dma((2,)),
        ],
        compiler_params=pltpu.CompilerParams(
            collective_id=0, has_side_effects=True, vmem_limit_bytes=60 * 2**20
        ),
        cost_estimate=pl.CostEstimate(flops=19 * 10**9, bytes_accessed=8 * 2**20, transcendentals=25 * 10**6),
    )(queries, key_vectors, value_vectors, out_weight, frame_mask)


def solution(mesh):
    in_specs = (
        P(("tm", "space"), None),
        P(("tm", "space"), None),
        P(("tm", "space"), None),
        P(None, "space"),
        P(),
    )
    return jax.shard_map(body, mesh=mesh, in_specs=in_specs, out_specs=P("tm", "space"), check_vma=False)
```

```python
import functools
import math

import jax
import jax.numpy as jnp
from jax import lax
from jax.experimental import pallas as pl
from jax.experimental.pallas import tpu as pltpu
from jax.sharding import PartitionSpec as P

MESH = pl.DeviceIdType.MESH
HD = 128
HEADS = 32
TOK = 128
BT = 2048
TQ = 256
KC = 512
COLS = 384
ROWS = 512
STEPS = 16
EARLY = 8
RELAY = 4
SLOPE = math.log2(math.e) / math.sqrt(HD)
BIG = 1e30


def place():
    tm = lax.axis_index("tm")
    sp = lax.axis_index("space")
    return tm, sp, tm // 2, tm % 2


def taken(ref, sem):
    pltpu.make_async_copy(ref, ref, sem).wait()


def attend(q, k_all, v_all, scores, blocks, known=None):
    chunks = BT // KC
    top = None
    for j, (base, bit) in enumerate(blocks):
        part = None
        for c in range(chunks):
            off = j * BT + c * KC
            s = lax.dot_general(
                q, k_all[pl.ds(base + c * KC, KC), :], (((1,), (1,)), ((), ())),
                preferred_element_type=jnp.float32,
            )
            scores[:, off:off + KC] = s
            for lane in range(0, KC, 128):
                piece = s[:, lane:lane + 128]
                part = piece if part is None else jnp.maximum(part, piece)
        if bit is not None:
            part = jnp.where(bit, part, -jnp.inf)
        top = part if top is None else jnp.maximum(top, part)
    top = jnp.max(top, axis=1, keepdims=True)
    acc = None
    total = None
    if known is not None:
        old_top, total, acc = known
        top = jnp.maximum(top, old_top[:, 0:1])
        shrink = jnp.exp2((old_top - top) * SLOPE)
        total = total * shrink
        acc = acc * shrink
    for j, (base, bit) in enumerate(blocks):
        sub = top if bit is None else jnp.where(bit, top, BIG)
        for c in range(chunks):
            off = j * BT + c * KC
            p = jnp.exp2((scores[:, off:off + KC] - sub) * SLOPE)
            for lane in range(0, KC, 128):
                piece = p[:, lane:lane + 128]
                total = piece if total is None else total + piece
            d = jnp.dot(
                p.astype(jnp.bfloat16), v_all[pl.ds(base + c * KC, KC), :],
                preferred_element_type=jnp.float32,
            )
            acc = d if acc is None else acc + d
    return top, total, acc


def finish(total, acc):
    return (acc / jnp.sum(total, axis=1, keepdims=True)).astype(jnp.bfloat16)


def kernel(
    q_hbm, k_hbm, v_hbm, w_hbm, mask_ref, out_ref,
    q_all, k_all, v_all, scores, att, got, w_all, done, tile_out, early_top, early_total, early_acc,
    sent, landed, passed_sem, came_sem, near_send, near_recv, far_send, far_recv, relay_recv,
    w_mine, w_send, w_recv, o_send, o_recv, o_own,
):
    tm, sp, y, xl = place()
    z = sp // 4
    xh = (sp // 2) % 2
    core = sp % 2
    me = xl * 16 + sp

    def at_y(step):
        return (((y + step) % 4) * 2 + xl, sp)

    def at_z(step):
        return (tm, ((z + step) % 4) * 4 + sp % 4)

    barrier = pltpu.get_barrier_semaphore()

    def greet(i, carry):
        p = (me + i) % 32
        pl.semaphore_signal(barrier, inc=1, device_id=(y * 2 + p // 16, p % 16), device_id_type=MESH)
        return carry

    lax.fori_loop(1, 32, greet, 0)
    for step in (1, 2, 3):
        pl.semaphore_signal(barrier, inc=1, device_id=at_y(step), device_id_type=MESH)
    pl.semaphore_wait(barrier, 34)

    mine = pl.ds(pl.multiple_of((sp * 2 + xl) * HD, HD), HD)
    plan = ((k_hbm, k_all, BT), (v_hbm, v_all, BT), (q_hbm, q_all, 0))
    cuts = (1, 16, 32)

    def rows_at(n):
        return pl.ds(pl.multiple_of(plan[n][2] + me * TOK, TOK), TOK)

    def send_part(n, part):
        hbm, dst, first = plan[n]

        def send(i, carry):
            p = (me + i) % 32
            theirs = pl.ds(pl.multiple_of(((p % 16) * 2 + p // 16) * HD, HD), HD)
            pltpu.make_async_remote_copy(
                src_ref=hbm.at[:, theirs], dst_ref=dst.at[rows_at(n), :],
                send_sem=sent.at[n, part], recv_sem=landed.at[n],
                device_id=(y * 2 + p // 16, p % 16), device_id_type=MESH,
            ).start()
            return carry

        lax.fori_loop(cuts[part], cuts[part + 1], send, 0)

    def sent_part(n, part):
        taken(q_all.at[0:(cuts[part + 1] - cuts[part]) * TOK, :], sent.at[n, part])

    hops = []

    def hop_on(n):
        buf = plan[n][1]
        taken(buf.at[BT:3 * BT, :], landed.at[n])
        for way, (step, src, dst) in enumerate(((1, 2 * BT, 0), (3, BT, 3 * BT))):
            hop = pltpu.make_async_remote_copy(
                src_ref=buf.at[src:src + BT, :], dst_ref=buf.at[dst:dst + BT, :],
                send_sem=passed_sem.at[2 * n + way], recv_sem=came_sem.at[2 * n + way],
                device_id=at_y(step), device_id_type=MESH,
            )
            hop.start()
            hops.append(hop)

    for n in range(3):
        pltpu.make_async_copy(plan[n][0].at[:, mine], plan[n][1].at[rows_at(n), :], landed.at[n]).start()
    send_part(0, 0)
    send_part(0, 1)
    for n in (0, 1):
        sent_part(n, 0)
        send_part(n + 1, 0)
        sent_part(n, 1)
        send_part(n + 1, 1)
        hop_on(n)

    def columns(n):
        return pl.ds(pl.multiple_of(n * COLS, COLS), COLS)

    near_cols = columns(2 + core)
    far_cols = columns(core)
    quarter = pl.ds(pl.multiple_of(y * 1024, 1024), 1024)
    g_me = xh * 2 + core
    partner = (tm, sp + 1 - 2 * core)
    across = (y * 2 + 1 - xl, z * 4 + (1 - xh) * 2 + core)
    w_first = pltpu.make_async_remote_copy(
        src_ref=w_hbm.at[quarter, :], dst_ref=w_all.at[quarter, far_cols],
        send_sem=w_send.at[1], recv_sem=w_recv.at[1], device_id=across, device_id_type=MESH,
    )
    w_first.start()
    w_own = pltpu.make_async_copy(w_hbm, w_all.at[:, near_cols], w_mine)
    w_own.start()
    w_near = pltpu.make_async_remote_copy(
        src_ref=w_hbm, dst_ref=w_all.at[:, near_cols], send_sem=w_send.at[0], recv_sem=w_recv.at[0],
        device_id=partner, device_id_type=MESH,
    )
    w_near.start()
    w_last = pltpu.make_async_remote_copy(
        src_ref=w_all.at[:, far_cols], dst_ref=w_all.at[:, far_cols],
        send_sem=w_send.at[3], recv_sem=w_recv.at[3], device_id=partner, device_id_type=MESH,
    )

    def spot(s):
        half = s % 2
        row = half * BT + ((s % 4) // 2 * 2 + (s % 8) // 4) * ROWS + s // 8 * TQ
        block = y * 2 + half
        before = mask_ref[block, (block + 7) % 8] == 1
        after = mask_ref[block, (block + 1) % 8] == 1
        return half, pl.ds(pl.multiple_of(row, TQ), TQ), before, after

    def early(s, carry):
        half, rows, before, after = spot(s)
        blocks = ((BT, (half == 0) | before), (2 * BT, (half == 1) | after))
        top, total, acc = attend(q_all[rows, :], k_all, v_all, scores, blocks)
        early_top[s] = jnp.broadcast_to(top, (TQ, HD))
        early_total[s] = total
        early_acc[s] = acc
        return carry

    taken(q_all, landed.at[2])
    lax.fori_loop(0, EARLY, early, 0)
    for hop in hops:
        hop.wait()
    sent_part(2, 0)
    sent_part(2, 1)

    turn = core * 4 + xh * 2 + xl
    slot = xh * 4 + core * 2 + xl

    def along_z(chunk):
        rows = pl.ds(chunk * TQ, TQ)
        taken(got.at[0, 0:7, 0:TQ, :], near_recv.at[chunk])
        for way, step in enumerate((1, 3)):
            pltpu.make_async_remote_copy(
                src_ref=got.at[z, :, rows, :], dst_ref=got.at[z, :, rows, :],
                send_sem=far_send, recv_sem=far_recv.at[2 * chunk + way],
                device_id=at_z(step), device_id_type=MESH,
            ).start()

    def relay_z(chunk):
        rows = pl.ds(chunk * TQ, TQ)
        for way, (come, step) in enumerate(((3, 1), (1, 3))):
            taken(got.at[0, :, 0:TQ, :], far_recv.at[2 * chunk + way])
            part = got.at[(z + come) % 4, 4 * way:4 * way + 4, rows, :]
            pltpu.make_async_remote_copy(
                src_ref=part, dst_ref=part, send_sem=far_send, recv_sem=relay_recv.at[chunk],
                device_id=at_z(step), device_id_type=MESH,
            ).start()

    def tile(s, carry):
        chunk = s // 8
        to_core = (s % 8) // 4
        half = s % 2
        to_xh = (s % 4) // 2
        _, rows, before, after = spot(s)
        base = pl.multiple_of(half * BT, BT)
        there = pl.ds(pl.multiple_of(chunk * TQ, TQ), TQ)

        @pl.when(s < EARLY)
        def _():
            n = jnp.minimum(s, EARLY - 1)
            last = pl.multiple_of(half * 3 * BT, BT)
            bit = ((half == 0) & before) | ((half == 1) & after)
            known = (early_top[n], early_total[n], early_acc[n])
            _, total, acc = attend(q_all[rows, :], k_all, v_all, scores, ((last, bit),), known)
            tile_out[...] = finish(total, acc)

        @pl.when(s >= EARLY)
        def _():
            blocks = ((base, before), (base + BT, None), (base + 2 * BT, after))
            _, total, acc = attend(q_all[rows, :], k_all, v_all, scores, blocks)
            tile_out[...] = finish(total, acc)

        result = tile_out[...]

        @pl.when(s % 8 == turn)
        def _():
            got[z, slot, there, :] = result

        @pl.when(s % 8 != turn)
        def _():
            att[rows, :] = result
            pltpu.make_async_remote_copy(
                src_ref=att.at[rows, :], dst_ref=got.at[z, slot, there, :],
                send_sem=near_send, recv_sem=near_recv.at[chunk],
                device_id=(y * 2 + half, z * 4 + to_xh * 2 + to_core), device_id_type=MESH,
            ).start()

        for c in (0, 1):
            @pl.when(s == c * 8 + turn + 1)
            def _(c=c):
                along_z(c)

            @pl.when(s == c * 8 + turn + RELAY)
            def _(c=c):
                relay_z(c)

        @pl.when(s == 2)
        def _():
            w_first.wait()
            for n, step in enumerate((1, 3, 2)):
                pltpu.make_async_remote_copy(
                    src_ref=w_all.at[quarter, far_cols], dst_ref=w_all.at[quarter, far_cols],
                    send_sem=w_send.at[2], recv_sem=w_recv.at[2], device_id=at_y(step), device_id_type=MESH,
                ).start()

        @pl.when(s == STEPS - 2)
        def _():
            taken(w_all.at[0:3072, 0:COLS], w_recv.at[2])
            w_last.start()

        return carry

    lax.fori_loop(0, STEPS, tile, 0)

    @pl.when(turn == 7)
    def _():
        along_z(1)

    w_own.wait()
    w_near.wait()
    w_last.wait()

    own_copies = []
    for chunk in (0, 1):
        rows = pl.ds(chunk * TQ, TQ)
        out_rows = pl.ds(pl.multiple_of(g_me * ROWS + chunk * TQ, TQ), TQ)

        def give(there, cols, chunk=chunk, out_rows=out_rows):
            pltpu.make_async_remote_copy(
                src_ref=done.at[chunk, :, cols], dst_ref=out_ref.at[out_rows, :],
                send_sem=o_send, recv_sem=o_recv,
                device_id=(tm, there), device_id_type=MESH,
            ).start()

        if chunk == 1:
            @pl.when(turn + 8 + RELAY > STEPS - 1)
            def _():
                relay_z(1)

        taken(got.at[0, :, 0:TQ, :], relay_recv.at[chunk])
        lhs = jnp.concatenate([got[i // 8, i % 8, rows, :] for i in range(HEADS)], axis=1)
        for n in range(3):
            wide = slice(n * 512, (n + 1) * 512)
            done[chunk, :, wide] = jnp.dot(lhs, w_all[:, wide], preferred_element_type=jnp.float32).astype(jnp.bfloat16)
            if n == 1:
                for c in (0, 1):
                    give(z * 4 + (1 - xh) * 2 + c, slice(c * COLS, (c + 1) * COLS))
        give(sp + 1 - 2 * core, columns(3 - core))
        own = pltpu.make_async_copy(done.at[chunk, :, near_cols], out_ref.at[out_rows, :], o_own.at[chunk])
        own.start()
        own_copies.append(own)

    for own in own_copies:
        own.wait()
    taken(done.at[:, :, 0:3 * COLS], o_recv)
    taken(done.at[:, :, 0:3 * COLS], o_send)
    taken(q_all.at[0:14 * TQ, :], near_send)
    taken(got.at[0:3], far_send)
    taken(w_all.at[0:3072, 0:COLS], w_send.at[2])


def body(queries, key_vectors, value_vectors, out_weight, frame_mask):
    hbm = pl.BlockSpec(memory_space=pl.ANY)
    dma = pltpu.SemaphoreType.DMA
    bf16 = jnp.bfloat16
    return pl.pallas_call(
        kernel,
        name="layer",
        out_shape=jax.ShapeDtypeStruct((BT, COLS), bf16),
        in_specs=[hbm] * 4 + [pl.BlockSpec(memory_space=pltpu.SMEM)],
        out_specs=hbm,
        scratch_shapes=[
            pltpu.VMEM((2 * BT, HD), bf16),
            pltpu.VMEM((4 * BT, HD), bf16),
            pltpu.VMEM((4 * BT, HD), bf16),
            pltpu.VMEM((TQ, 3 * BT), jnp.float32),
            pltpu.VMEM((2 * BT, HD), bf16),
            pltpu.VMEM((4, 8, ROWS, HD), bf16),
            pltpu.VMEM((HEADS * HD, 4 * COLS), bf16),
            pltpu.VMEM((2, TQ, 4 * COLS), bf16),
            pltpu.VMEM((TQ, HD), bf16),
            pltpu.VMEM((EARLY, TQ, HD), jnp.float32),
            pltpu.VMEM((EARLY, TQ, HD), jnp.float32),
            pltpu.VMEM((EARLY, TQ, HD), jnp.float32),
            dma((3, 2)), dma((3,)), dma((4,)), dma((4,)), dma, dma((2,)), dma, dma((4,)), dma((2,)),
            dma, dma((4,)), dma((4,)), dma, dma, dma((2,)),
        ],
        compiler_params=pltpu.CompilerParams(
            collective_id=0, has_side_effects=True, vmem_limit_bytes=60 * 2**20
        ),
        cost_estimate=pl.CostEstimate(flops=19 * 10**9, bytes_accessed=8 * 2**20, transcendentals=25 * 10**6),
    )(queries, key_vectors, value_vectors, out_weight, frame_mask)


def solution(mesh):
    in_specs = (
        P(("tm", "space"), None),
        P(("tm", "space"), None),
        P(("tm", "space"), None),
        P(None, "space"),
        P(),
    )
    return jax.shard_map(body, mesh=mesh, in_specs=in_specs, out_specs=P("tm", "space"), check_vma=False)
```
